32 devices in a mesh: dev: 32 (over z, y, x, core).
Axes of the slice: x: 2, y: 2, z: 4, core: 2. Of those that a mesh axis runs over, the one named last changes fastest.
Arguments:
- pixels: bfloat16 [96, 64, 16], P('dev'), may hold values from -6 to 6
- embed_w: bfloat16 [96, 16, 8192], P('dev'), may hold values from -1.5 to 1.5
- var_embed: bfloat16 [96, 8192], P('dev'), may hold values from -3 to 3
- key_w: bfloat16 [8192, 8192], P('dev'), may hold values from -0.0625 to 0.0625
- query: float32 [8192], replicated, may hold values from -500 to 500
- value_t: bfloat16 [8192, 8192], P('dev'), may hold values from -0.0625 to 0.0625
- out_w: bfloat16 [8192, 8192], P('dev'), may hold values from -0.0625 to 0.0625
Outputs:
- mixed: bfloat16 [64, 8192], P('dev')
The draws below stay inside these ranges and needn't reach their ends.
All inputs are finite; a program needn't handle non-finite values.
Results may differ from the reference program's by a relative error of at most 0.012.
The reference program's roundings to bfloat16 on the way (of `embed`, `attn`, `pooled` and `heads`) count: a program that leaves them out, or rounds other values in their place, can miss the bound.
Values may be sent and summed in bfloat16 or wider, within the bound.
A program may use at most 64 MiB of HBM per device.

```python
import jax
import jax.numpy as jnp
from jax import lax

D = 8192
HEADS = 64
HD = 128
P_SIZE = 16
V = 91
TOK_DEV = 2
VSLOT = 96
TOKENS = 64
N_DEV = 32


def draw_query(key, part):
    first, second = jax.random.split(jax.random.fold_in(key, 17))
    base = jnp.clip(jax.random.normal(first, (HEADS, HD), jnp.float32), -5.0, 5.0)
    scales = jnp.exp(jax.random.uniform(second, (HEADS, 1), jnp.float32, jnp.log(0.5), jnp.log(3.0)))
    return (base * scales).reshape(HEADS * HD)


def steps_of(key, shape, cuts, low, largest):
    gain = 1.0
    for dim, shards_of in cuts:
        heights = jax.random.uniform(jax.random.fold_in(jax.random.fold_in(key, 6), dim), (shards_of,), jnp.float32, low / len(cuts), largest / len(cuts))
        gain = gain * jnp.repeat(jnp.exp(heights), shape[dim] // shards_of).reshape((-1,) + (1,) * (len(shape) - 1 - dim))
    return gain


def bell_draw(own_key, shape, deviation, reach, shards=(), held_as=jnp.bfloat16):
    array = deviation * jax.random.normal(own_key, shape, jnp.float32)
    if shards:
        array = array * steps_of(own_key, shape, shards, -0.22, 0.18)
    return jnp.clip(array, -reach, reach).astype(held_as)


def setup_inputs(seed: int = 0) -> dict:
    key_of = jax.random.split(jax.random.key(seed), 8)
    pixels = bell_draw(key_of[0], (VSLOT, TOKENS, P_SIZE), 1.0, 6.0, ((0, 32),))
    embed_w = bell_draw(key_of[1], (VSLOT, P_SIZE, D), P_SIZE ** -0.5, 1.5, ((0, 32),))
    var_embed = bell_draw(key_of[2], (VSLOT, D), 0.5, 3.0, ((0, 32),))
    key_w = bell_draw(key_of[3], (D, D), D ** -0.5, 0.0625, ((0, 32),))
    query = draw_query(jax.random.fold_in(key_of[7], 71), 0)
    value_t = bell_draw(key_of[5], (D, D), D ** -0.5, 0.0625, ((0, 32),))
    out_w = bell_draw(key_of[6], (D, D), D ** -0.5, 0.0625, ((0, 32),))
    return {"pixels": pixels, "embed_w": embed_w, "var_embed": var_embed, "key_w": key_w, "query": query, "value_t": value_t, "out_w": out_w}


def reference(pixels, embed_w, var_embed, key_w, query, value_t, out_w):
    query_heads = query.reshape(HEADS, HD)
    keyq = jnp.einsum('dhj,hj->dh', key_w.astype(jnp.float32).reshape(D, HEADS, HD), query_heads, precision=lax.Precision.HIGHEST)
    value_full = value_t.astype(jnp.float32).reshape(HEADS, HD, D)
    live_pixels = pixels[:V].reshape(V, N_DEV, TOK_DEV, P_SIZE).transpose(1, 0, 2, 3)
    live_embed_w = embed_w[:V].astype(jnp.float32)
    live_var = var_embed[:V].astype(jnp.float32)

    def one_block(block):
        embed = jnp.einsum('vtp,vpd->vtd', block.astype(jnp.float32), live_embed_w, precision=lax.Precision.HIGHEST)
        embed = (embed + live_var[:, None, :]).astype(jnp.bfloat16)
        logits = jnp.einsum('vtd,dh->vth', embed.astype(jnp.float32), keyq, precision=lax.Precision.HIGHEST) / jnp.sqrt(jnp.float32(HD))
        row_max = lax.optimization_barrier(jnp.max(logits, axis=0, keepdims=True))
        weights = jnp.exp(logits - row_max)
        attn = (weights / lax.optimization_barrier(jnp.sum(weights, axis=0, keepdims=True))).astype(jnp.bfloat16)
        pooled = jnp.einsum('vth,vtd->thd', attn.astype(jnp.float32), embed.astype(jnp.float32), precision=lax.Precision.HIGHEST).astype(jnp.bfloat16)
        heads = jnp.einsum('thd,hcd->thc', pooled.astype(jnp.float32), value_full, precision=lax.Precision.HIGHEST)
        heads = heads.reshape(TOK_DEV, D).astype(jnp.bfloat16)
        return jnp.dot(heads, out_w, preferred_element_type=jnp.float32).astype(jnp.bfloat16)
    mixed = lax.map(one_block, live_pixels)
    return mixed.reshape(TOKENS, D)
```

```python
import functools

import jax
import jax.numpy as jnp
from jax import lax
from jax.experimental import pallas as pl
from jax.experimental.pallas import tpu as pltpu
from jax.sharding import PartitionSpec as P

D = 8192
HEADS = 64
HD = 128
V = 91
CH = 16
MESH = pl.DeviceIdType.MESH
F32 = jnp.float32
BF16 = jnp.bfloat16


def fallback_tail(grouped, attn, value_t, out_w, group_size):
    pooled = jnp.einsum("vth,vtd->thd", attn, grouped, preferred_element_type=F32).astype(BF16)
    own_tokens = pooled.shape[0]
    if group_size >= HEADS:
        spread = jnp.repeat(pooled, group_size // HEADS, axis=1)[:, :, None, :]
    else:
        spread = pooled.reshape(own_tokens, group_size, HEADS // group_size, D)
    received = lax.all_to_all(spread, "dev", split_axis=1, concat_axis=0, tiled=True)
    all_tokens = received.shape[0]
    head_share = received.shape[2]
    received = received.reshape(all_tokens, head_share, D)
    columns = value_t.shape[0]
    value_heads = jnp.einsum(
        "thd,hcd->thc",
        received,
        value_t.reshape(head_share, columns // head_share, D),
        preferred_element_type=F32,
    )
    value_heads = value_heads.reshape(all_tokens, columns).astype(BF16)
    summed = lax.psum_scatter(
        jnp.dot(value_heads, out_w, preferred_element_type=F32),
        "dev",
        scatter_dimension=0,
        tiled=True,
    )
    return summed.astype(BF16)


def softmax_slots(logits):
    slot = lax.broadcasted_iota(jnp.int32, logits.shape, 0)
    logits = jnp.where(slot < V, logits, -1e30)
    row_max = jnp.max(logits, axis=0, keepdims=True)
    weights = jnp.exp(logits - row_max)
    return (weights / jnp.sum(weights, axis=0, keepdims=True)).astype(BF16)


def tail_kernel(
    n, pix, w, var, attn, value_hbm, out_hbm, result,
    embf, pf, pool, got, vbuf, obuf, part, rc, r1, r2, ysum, rz, fbuf, gbuf,
    wsem, psend, precv, csend, crecv, s1send, s1recv, s2send, s2recv, zsend, zrecv, fsend, frecv,
):
    me = lax.axis_index("dev")
    core, x, y, z = me % 2, (me // 2) % 2, (me // 4) % 2, me // 8
    nz = n // 8
    slots, tokens, _ = pix.shape
    dl = w.shape[2]
    lanes = dl // 128
    hs = HEADS // n
    chunks = tokens // CH
    take = hs * CH
    load_v = pltpu.make_async_copy(value_hbm, vbuf, wsem.at[0])
    load_o = pltpu.make_async_copy(out_hbm, obuf, wsem.at[1])
    load_v.start()
    load_o.start()

    def embed_one(v, carry):
        e = jnp.dot(pix[v], w[v], preferred_element_type=F32) + var[v]
        e = e.astype(BF16).astype(F32)
        for k in range(lanes):
            embf[k, pl.ds(v, tokens, stride=slots), :] = e[:, k * 128:(k + 1) * 128]
        return carry

    lax.fori_loop(0, slots, embed_one, 0, unroll=4)

    def exchange(c, partner, slot):
        return pltpu.make_async_remote_copy(
            src_ref=pool.at[c, pl.ds(pl.multiple_of(partner * take, 16), take), :],
            dst_ref=got.at[slot, c],
            send_sem=psend.at[c, partner],
            recv_sem=precv.at[c, slot],
            device_id=(partner,),
            device_id_type=MESH,
        )

    for c in range(chunks):
        def pool_one(tt, carry, c=c):
            t = c * CH + tt
            row = pl.ds(pl.multiple_of(t * slots, 8), slots)
            em = jnp.concatenate([embf[k, row, :] for k in range(lanes)], axis=1).astype(BF16)
            p = lax.dot_general(attn[t], em, (((0,), (0,)), ((), ())), preferred_element_type=F32)
            for k in range(lanes):
                pf[k, pl.ds(tt, HEADS, stride=CH), :] = p[:, k * 128:(k + 1) * 128]
            return carry

        lax.fori_loop(0, CH, pool_one, 0, unroll=2)

        def pack(i, carry, c=c):
            rows = pl.ds(pl.multiple_of(i * 64, 64), 64)
            pool[c, rows, :] = jnp.concatenate([pf[k, rows, :] for k in range(lanes)], axis=1).astype(BF16)
            return carry

        lax.fori_loop(0, HEADS * CH // 64, pack, 0)
        got[me, c] = pool[c, pl.ds(pl.multiple_of(me * take, 16), take), :]

        def send(i, carry, c=c):
            exchange(c, (me + n // 2 + i) % n, me).start()
            return carry

        lax.fori_loop(0, n // 2, send, 0)
        lax.fori_loop(n // 2 + 1, n, send, 0)

    load_v.wait()

    def value_one(i, accs):
        s = (me + i) % n
        block = got[s]
        cols = pl.ds(pl.multiple_of(s * dl, 128), dl)
        new = []
        for h in range(hs):
            r = block[:, h * CH:(h + 1) * CH, :].reshape(tokens, dl)
            vv = vbuf[h * HD:(h + 1) * HD, cols]
            new.append(accs[h] + lax.dot_general(r, vv, (((1,), (1,)), ((), ())), preferred_element_type=F32))
        return tuple(new)

    def arrive_one(i, accs):
        s = (me + i) % n
        for c in range(chunks):
            pltpu.make_async_remote_copy(
                src_ref=got.at[s, c], dst_ref=got.at[s, c], send_sem=psend.at[c, s],
                recv_sem=precv.at[c, s], device_id=(s,), device_id_type=MESH,
            ).wait_recv()
        return value_one(i, accs)

    accs = value_one(0, tuple(jnp.zeros((tokens, HD), F32) for _ in range(hs)))
    accs = lax.fori_loop(1, n, arrive_one, accs)
    heads = jnp.concatenate(accs, axis=1).astype(BF16)

    load_o.wait()
    wide = D // 8
    half_w = wide // 2

    def out_blocks(cc, half):
        for a in range(2):
            for b in range(2):
                q = cc + 2 * (a if half == 0 else b) + 4 * (b if half == 0 else a)
                col = pl.multiple_of(q * wide + half * half_w, 128)
                part[cc, half, a, b] = jnp.dot(heads, obuf[:, pl.ds(col, half_w)], preferred_element_type=F32)

    def remote(src, dst, ss, rs, dev):
        return pltpu.make_async_remote_copy(
            src_ref=src, dst_ref=dst, send_sem=ss, recv_sem=rs, device_id=(dev,), device_id_type=MESH
        )

    other = me + 1 - 2 * core
    xn = me + 2 * (1 - 2 * x)
    yn = me + 4 * (1 - 2 * y)
    core_copies = []
    for half in range(2):
        out_blocks(1 - core, half)
        cp = remote(part.at[1 - core, half], rc.at[half], csend.at[half], crecv.at[half], other)
        cp.start()
        core_copies.append(cp)
    for half in range(2):
        out_blocks(core, half)
    first = (x, y)
    second = (y, x)
    first_dev = (xn, yn)
    second_dev = (yn, xn)
    stage1 = []
    for half in range(2):
        core_copies[half].wait_recv()
        away = 1 - first[half]
        for b in range(2):
            part[core, half, away, b] = part[core, half, away, b] + rc[half, away, b]
        cp = remote(part.at[core, half, away], r1.at[half], s1send.at[half], s1recv.at[half], first_dev[half])
        cp.start()
        stage1.append(cp)
    for half in range(2):
        own = first[half]
        for b in range(2):
            part[core, half, own, b] = part[core, half, own, b] + rc[half, own, b]
    stage2 = []
    for half in range(2):
        own = first[half]
        stage1[half].wait_recv()
        away = 1 - second[half]
        part[core, half, own, away] = part[core, half, own, away] + r1[half, away]
        cp = remote(part.at[core, half, own, away], r2.at[half], s2send.at[half], s2recv.at[half], second_dev[half])
        cp.start()
        stage2.append(cp)
    for half in range(2):
        own, mine = first[half], second[half]
        kept = part[core, half, own, mine] + r1[half, mine]
        stage2[half].wait_recv()
        ysum[half] = kept + r2[half]
    rows_z = tokens // nz
    zcopies = []
    for dz in range(1, nz):
        zz = (z + dz) % nz
        cp = remote(
            ysum.at[:, pl.ds(pl.multiple_of(zz * rows_z, 8), rows_z), :],
            rz.at[dz - 1], zsend.at[dz - 1], zrecv.at[dz - 1], me + 8 * (zz - z),
        )
        cp.start()
        zcopies.append(cp)
    total = ysum[:, pl.ds(pl.multiple_of(z * rows_z, 8), rows_z), :]
    for dz in range(1, nz):
        zcopies[dz - 1].wait_recv()
        total = total + rz[dz - 1]
    tok = tokens // n
    for k in range(8):
        for half in range(2):
            fbuf[k, :, half * half_w:(half + 1) * half_w] = total[half, k * tok:(k + 1) * tok, :]
    q = me % 8
    fcopies = []
    for dk in range(1, 8):
        k = (q + dk) % 8
        cp = remote(fbuf.at[k], gbuf.at[q], fsend.at[k], frecv.at[q], me - q + k)
        cp.start()
        fcopies.append(cp)
    gbuf[q] = fbuf[q]
    for dk in range(1, 8):
        k = (q + dk) % 8
        remote(gbuf.at[k], gbuf.at[k], fsend.at[k], frecv.at[k], me - q + k).wait_recv()
    for k in range(8):
        result[:, k * wide:(k + 1) * wide] = gbuf[k].astype(BF16)

    for group in (core_copies, stage1, stage2, zcopies, fcopies):
        for cp in group:
            cp.wait_send()

    def drain(i, carry):
        for c in range(chunks):
            exchange(c, (me + i) % n, me).wait_send()
        return carry

    lax.fori_loop(1, n, drain, 0)


def fused_tail(n, pix, w, var, attn, value_t, out_w):
    slots, tokens, _ = pix.shape
    dl = w.shape[2]
    lanes = dl // 128
    hs = HEADS // n
    chunks = tokens // CH
    nz = n // 8
    wide = D // 8
    half_w = wide // 2
    tok = tokens // n
    dma = pltpu.SemaphoreType.DMA
    vmem = pl.BlockSpec(memory_space=pltpu.VMEM)
    hbm = pl.BlockSpec(memory_space=pl.ANY)
    return pl.pallas_call(
        functools.partial(tail_kernel, n),
        out_shape=jax.ShapeDtypeStruct((tok, D), BF16),
        in_specs=[vmem] * 4 + [hbm] * 2,
        out_specs=vmem,
        scratch_shapes=[
            pltpu.VMEM((lanes, tokens * slots, 128), F32),
            pltpu.VMEM((lanes, HEADS * CH, 128), F32),
            pltpu.VMEM((chunks, HEADS * CH, dl), BF16),
            pltpu.VMEM((n, chunks, hs * CH, dl), BF16),
            pltpu.VMEM(value_t.shape, BF16),
            pltpu.VMEM(out_w.shape, BF16),
            pltpu.VMEM((2, 2, 2, 2, tokens, half_w), F32),
            pltpu.VMEM((2, 2, 2, tokens, half_w), F32),
            pltpu.VMEM((2, 2, tokens, half_w), F32),
            pltpu.VMEM((2, tokens, half_w), F32),
            pltpu.VMEM((2, tokens, half_w), F32),
            pltpu.VMEM((nz - 1, 2, tokens // nz, half_w), F32),
            pltpu.VMEM((8, tok, wide), F32),
            pltpu.VMEM((8, tok, wide), F32),
            dma((2,)), dma((chunks, n)), dma((chunks, n)),
            dma((2,)), dma((2,)), dma((2,)), dma((2,)), dma((2,)), dma((2,)),
            dma((nz - 1,)), dma((nz - 1,)), dma((8,)), dma((8,)),
        ],
        compiler_params=pltpu.CompilerParams(
            has_side_effects=True, vmem_limit_bytes=60 * 1024 * 1024
        ),
    )(pix, w, var, attn, value_t, out_w)


def body(pixels, embed_w, var_embed, key_w, query, value_t, out_w):
    n = lax.axis_size("dev")
    own_slots, tokens, _ = pixels.shape
    own_embed = jnp.einsum("vtp,vpd->vtd", pixels, embed_w, preferred_element_type=F32)
    own_embed = (own_embed + var_embed.astype(F32)[:, None, :]).astype(BF16)
    key_rows = key_w.shape[0]
    keyq_part = jnp.einsum(
        "dhj,hj->dh",
        key_w.astype(F32).reshape(key_rows, HEADS, HD),
        query.reshape(HEADS, HD),
        precision=lax.Precision.HIGHEST,
    )
    keyq = lax.all_gather(keyq_part, "dev", axis=0, tiled=True)
    scale = jnp.sqrt(F32(HD))
    if n % 8 or n // 8 < 2 or HEADS % n or D // n % 128 or tokens % (8 * (n // 8)) or tokens % CH:
        grouped = lax.all_to_all(own_embed, "dev", split_axis=1, concat_axis=0, tiled=True)
        logits = jnp.einsum(
            "vtd,dh->vth", grouped.astype(F32), keyq, precision=lax.Precision.HIGHEST
        ) / scale
        return fallback_tail(grouped, softmax_slots(logits), value_t, out_w, n)
    weights = jnp.concatenate([embed_w, var_embed[:, None, :]], axis=1)
    weights = lax.all_to_all(weights, "dev", split_axis=2, concat_axis=0, tiled=True)
    all_pixels = lax.all_gather(pixels, "dev", axis=0, tiled=True)
    own_logits = jnp.einsum(
        "vtd,dh->vth", own_embed.astype(F32), keyq, precision=lax.Precision.HIGHEST
    ) / scale
    logits = lax.all_gather(own_logits, "dev", axis=0, tiled=True)
    attn = jnp.swapaxes(softmax_slots(logits), 0, 1)
    patch = pixels.shape[2]
    return fused_tail(
        n, all_pixels, weights[:, :patch, :], weights[:, patch:, :].astype(F32), attn, value_t, out_w
    )


def solution(mesh):
    placed = (
        P("dev", None, None),
        P("dev", None, None),
        P("dev", None),
        P("dev", None),
        P(),
        P("dev", None),
        P("dev", None),
    )
    return jax.shard_map(
        body, mesh=mesh, in_specs=placed, out_specs=P("dev", None), check_vma=False
    )
```

```python
import functools

import jax
import jax.numpy as jnp
from jax import lax
from jax.experimental import pallas as pl
from jax.experimental.pallas import tpu as pltpu
from jax.sharding import PartitionSpec as P

D = 8192
HEADS = 64
HD = 128
V = 91
CH = 16
EARLY = 8
MESH = pl.DeviceIdType.MESH
F32 = jnp.float32
BF16 = jnp.bfloat16


def remote(src, dst, ss, rs, dev):
    return pltpu.make_async_remote_copy(
        src_ref=src, dst_ref=dst, send_sem=ss, recv_sem=rs, device_id=(dev,), device_id_type=MESH
    )


def slot_of(s, nz):
    return (s % 2 * 4 + (s // 4) % 2 * 2 + (s // 2) % 2) * nz + s // 8


def gather_steps(buf, send, recv, me, nz):
    core, x, y, z = me % 2, (me // 2) % 2, (me // 4) % 2, me // 8
    q, qx, qy, qd = (
        core * 4 + yy * 2 + xx for yy, xx in ((y, x), (y, 1 - x), (1 - y, x), (1 - y, 1 - x))
    )
    xn, yn, other = me + 2 * (1 - 2 * x), me + 4 * (1 - 2 * y), me + 1 - 2 * core
    started = []

    def go(k, block, dev):
        cp = remote(block, block, send.at[k], recv.at[k], dev)
        cp.start()
        started.append(cp)
        return cp

    def along_z():
        for dz in range(1, nz):
            go(dz - 1, buf.at[q * nz + z], me + 8 * ((z + dz) % nz - z))

    def rest():
        for dz in range(1, nz):
            started[dz - 1].wait_recv()
        k = nz - 1
        half = nz // 2
        own = buf.at[pl.ds(q * nz, nz)]
        cx = go(k, own, xn)
        cy = go(k + 1, own, yn)
        c0 = go(k + 2, own, other)
        cx.wait_recv()
        fy = go(k + 3, buf.at[pl.ds(qx * nz, half)], yn)
        c1 = go(k + 5, buf.at[pl.ds(qx * nz, nz)], other)
        cy.wait_recv()
        fx = go(k + 4, buf.at[pl.ds(qy * nz + half, nz - half)], xn)
        c2 = go(k + 6, buf.at[pl.ds(qy * nz, nz)], other)
        return fy, fx, c0, c1, c2

    def finish(fy, fx, c0, c1, c2):
        fy.wait_recv()
        fx.wait_recv()
        c3 = go(nz + 6, buf.at[pl.ds(qd * nz, nz)], other)
        for cp in (c0, c1, c2, c3):
            cp.wait_recv()
        for cp in started:
            cp.wait_send()

    return along_z, rest, finish


def tail_kernel(
    n, pix, wp, var, qtile, key_hbm, value_hbm, out_hbm, result,
    kbuf, kq, wall, vall, oemb, lg, prob,
    embf, pf, pool, got, vbuf, obuf, part, rc, r1, r2, ysum, rz, fbuf, gbuf,
    gsend, grecv, hsend, hrecv, wsnd, wrcv, vsnd, vrcv, ksem,
    wsem, psend, precv, csend, crecv, s1send, s1recv, s2send, s2recv, zsend, zrecv, fsend, frecv,
):
    me = lax.axis_index("dev")
    core, x, y, z = me % 2, (me // 2) % 2, (me // 4) % 2, me // 8
    nz = n // 8
    vs, tokens, patch = pix.shape
    slots = n * vs
    dl = D // n
    lanes = dl // 128
    hs = HEADS // n
    chunks = tokens // CH
    take = hs * CH
    ht = tokens // 2
    mine = slot_of(me, nz)
    load_k = pltpu.make_async_copy(key_hbm, kbuf, ksem.at[0])
    load_k.start()
    load_v = pltpu.make_async_copy(value_hbm, vbuf, wsem.at[0])
    load_o = pltpu.make_async_copy(out_hbm, obuf, wsem.at[1])

    def cols_of(s):
        return pl.ds(pl.multiple_of(s * dl, 128), dl)

    def w_copy(partner, src):
        return remote(wp.at[:, :, cols_of(partner)], wall.at[src], wsnd.at[partner], wrcv.at[src], partner)

    def v_copy(partner, src):
        return remote(var.at[:, :, cols_of(partner)], vall.at[src], vsnd.at[partner], vrcv.at[src], partner)

    def w_send(i, carry):
        partner = (me + n // 2 + i) % n
        w_copy(partner, me).start()
        v_copy(partner, me).start()
        return carry

    early = EARLY
    lax.fori_loop(0, early, w_send, 0)
    load_k.wait()
    load_v.start()
    load_o.start()
    for kt in range(HEADS // 2):
        r = lax.dot_general(
            qtile[kt], kbuf[:, kt * 2 * HD:(kt + 1) * 2 * HD], (((1,), (1,)), ((), ())),
            preferred_element_type=F32,
        )
        kq[mine, 2 * kt:2 * kt + 2, :] = r[0:2] + r[2:4] + r[4:6]
    kq_z, kq_rest, kq_finish = gather_steps(kq, gsend, grecv, me, nz)
    lg_z, lg_rest, lg_finish = gather_steps(lg, hsend, hrecv, me, nz)
    kq_z()

    def own_one(s, carry):
        cols = cols_of(s)
        for v in range(vs):
            e = jnp.dot(pix[v], wp[v, :, cols], preferred_element_type=F32) + var[v, :, cols]
            oemb[v * tokens:(v + 1) * tokens, cols] = e.astype(BF16)
        return carry

    lax.fori_loop(0, n // 2, own_one, 0)
    state = kq_rest()
    lax.fori_loop(n // 2, n, own_one, 0)
    wall[me] = wp[:, :, cols_of(me)]
    vall[me] = var[:, :, cols_of(me)]
    kq_finish(*state)
    lax.fori_loop(early, n // 2, w_send, 0)
    lax.fori_loop(n // 2 + 1, n, w_send, 0)

    def logit_one(s, acc):
        a = kq[slot_of(s, nz)]
        hi = a.astype(BF16)
        rest = a - hi.astype(F32)
        mid = rest.astype(BF16)
        low = (rest - mid.astype(F32)).astype(BF16)
        b = jnp.concatenate([hi, mid, low], axis=0)
        return acc + lax.dot_general(
            oemb[:, cols_of(s)], b, (((1,), (1,)), ((), ())), preferred_element_type=F32
        )

    acc = lax.fori_loop(0, n, logit_one, jnp.zeros((vs * tokens, 3 * HEADS), F32))
    logit = (acc[:, :HEADS] + acc[:, HEADS:2 * HEADS] + acc[:, 2 * HEADS:]) / jnp.sqrt(F32(HD))
    for v in range(vs):
        pair = jnp.concatenate(
            [logit[v * tokens:v * tokens + ht], logit[v * tokens + ht:(v + 1) * tokens]], axis=1
        )
        live = jnp.full(pair.shape, me * vs + v, jnp.int32) < V
        lg[mine, v * ht:(v + 1) * ht, :] = jnp.where(live, pair, -1e30)
    lg_z()

    def embed_one(s):
        ps = jnp.transpose(wall[s, vs].astype(F32)).astype(BF16)
        at = slot_of(s, nz) * vs
        for v in range(vs):
            e = jnp.dot(ps[v * tokens:(v + 1) * tokens], wall[s, v], preferred_element_type=F32) + vall[s, v]
            e = e.astype(BF16).astype(F32)
            for k in range(lanes):
                embf[k, pl.ds(at + v, tokens, stride=slots), :] = e[:, k * 128:(k + 1) * 128]

    def arrive_w(i, carry):
        s = (me + i) % n
        w_copy(s, s).wait_recv()
        v_copy(s, s).wait_recv()
        embed_one(s)
        return carry

    embed_one(me)
    state = lg_rest()
    lax.fori_loop(1, n, arrive_w, 0)
    lg_finish(*state)
    for g in range(ht // 8):
        def at_v(v, g=g):
            return lg[v // vs, pl.ds(pl.multiple_of(v % vs * ht + g * 8, 8), 8), :]

        top = lax.fori_loop(1, slots, lambda v, m: jnp.maximum(m, at_v(v)), at_v(0), unroll=4)

        def exp_one(v, total, g=g, at_v=at_v, top=top):
            e = jnp.exp(at_v(v) - top)
            prob[pl.ds(pl.multiple_of(v * ht + g * 8, 8), 8), :] = e
            return total + e

        total = lax.fori_loop(0, slots, exp_one, jnp.zeros((8, 128), F32), unroll=4)

        def div_one(v, carry, g=g, total=total):
            rows = pl.ds(pl.multiple_of(v * ht + g * 8, 8), 8)
            prob[rows, :] = prob[rows, :] / total
            return carry

        lax.fori_loop(0, slots, div_one, 0, unroll=4)

    def exchange(c, partner, slot):
        return pltpu.make_async_remote_copy(
            src_ref=pool.at[c, pl.ds(pl.multiple_of(partner * take, 16), take), :],
            dst_ref=got.at[slot, c],
            send_sem=psend.at[c, partner],
            recv_sem=precv.at[c, slot],
            device_id=(partner,),
            device_id_type=MESH,
        )

    for c in range(chunks):
        def pool_one(tt, carry, c=c):
            t = c * (CH // 2) + tt
            at = prob[pl.ds(t, slots, stride=ht), :].astype(BF16)
            for side in range(2):
                row = pl.ds(pl.multiple_of((t + side * ht) * slots, 8), slots)
                em = jnp.concatenate([embf[k, row, :] for k in range(lanes)], axis=1).astype(BF16)
                p = lax.dot_general(
                    at[:, side * HEADS:(side + 1) * HEADS], em, (((0,), (0,)), ((), ())),
                    preferred_element_type=F32,
                )
                for k in range(lanes):
                    pf[k, pl.ds(tt + side * (CH // 2), HEADS, stride=CH), :] = p[:, k * 128:(k + 1) * 128]
            return carry

        lax.fori_loop(0, CH // 2, pool_one, 0, unroll=2)

        def pack(i, carry, c=c):
            rows = pl.ds(pl.multiple_of(i * 64, 64), 64)
            pool[c, rows, :] = jnp.concatenate([pf[k, rows, :] for k in range(lanes)], axis=1).astype(BF16)
            return carry

        lax.fori_loop(0, HEADS * CH // 64, pack, 0)
        got[me, c] = pool[c, pl.ds(pl.multiple_of(me * take, 16), take), :]

        def send(i, carry, c=c):
            exchange(c, (me + n // 2 + i) % n, me).start()
            return carry

        lax.fori_loop(0, n // 2, send, 0)
        lax.fori_loop(n // 2 + 1, n, send, 0)

    load_v.wait()

    def value_one(i, accs):
        s = (me + i) % n
        block = got[s]
        cols = pl.ds(pl.multiple_of(s * dl, 128), dl)
        new = []
        for h in range(hs):
            r = block[:, h * CH:(h + 1) * CH, :].reshape(tokens, dl)
            vv = vbuf[h * HD:(h + 1) * HD, cols]
            new.append(accs[h] + lax.dot_general(r, vv, (((1,), (1,)), ((), ())), preferred_element_type=F32))
        return tuple(new)

    def arrive_one(i, accs):
        s = (me + i) % n
        for c in range(chunks):
            pltpu.make_async_remote_copy(
                src_ref=got.at[s, c], dst_ref=got.at[s, c], send_sem=psend.at[c, s],
                recv_sem=precv.at[c, s], device_id=(s,), device_id_type=MESH,
            ).wait_recv()
        return value_one(i, accs)

    accs = value_one(0, tuple(jnp.zeros((tokens, HD), F32) for _ in range(hs)))
    accs = lax.fori_loop(1, n, arrive_one, accs)
    heads = jnp.concatenate(accs, axis=1)
    hc = CH // 2
    heads = jnp.concatenate(
        [heads[c * CH + side * hc:c * CH + (side + 1) * hc] for side in range(2) for c in range(chunks)], axis=0
    ).astype(BF16)

    load_o.wait()
    wide = D // 8
    half_w = wide // 2

    def out_blocks(cc, half):
        for a in range(2):
            for b in range(2):
                q = cc + 2 * (a if half == 0 else b) + 4 * (b if half == 0 else a)
                col = pl.multiple_of(q * wide + half * half_w, 128)
                part[cc, half, a, b] = jnp.dot(heads, obuf[:, pl.ds(col, half_w)], preferred_element_type=F32)

    other = me + 1 - 2 * core
    xn = me + 2 * (1 - 2 * x)
    yn = me + 4 * (1 - 2 * y)
    core_copies = []
    for half in range(2):
        out_blocks(1 - core, half)
        cp = remote(part.at[1 - core, half], rc.at[half], csend.at[half], crecv.at[half], other)
        cp.start()
        core_copies.append(cp)
    for half in range(2):
        out_blocks(core, half)
    first = (x, y)
    second = (y, x)
    first_dev = (xn, yn)
    second_dev = (yn, xn)
    stage1 = []
    for half in range(2):
        core_copies[half].wait_recv()
        away = 1 - first[half]
        for b in range(2):
            part[core, half, away, b] = part[core, half, away, b] + rc[half, away, b]
        cp = remote(part.at[core, half, away], r1.at[half], s1send.at[half], s1recv.at[half], first_dev[half])
        cp.start()
        stage1.append(cp)
    for half in range(2):
        own = first[half]
        for b in range(2):
            part[core, half, own, b] = part[core, half, own, b] + rc[half, own, b]
    stage2 = []
    for half in range(2):
        own = first[half]
        stage1[half].wait_recv()
        away = 1 - second[half]
        part[core, half, own, away] = part[core, half, own, away] + r1[half, away]
        cp = remote(part.at[core, half, own, away], r2.at[half], s2send.at[half], s2recv.at[half], second_dev[half])
        cp.start()
        stage2.append(cp)
    for half in range(2):
        own, kept_b = first[half], second[half]
        kept = part[core, half, own, kept_b] + r1[half, kept_b]
        stage2[half].wait_recv()
        ysum[half] = kept + r2[half]
    rows_z = tokens // nz
    zcopies = []
    for dz in range(1, nz):
        zz = (z + dz) % nz
        cp = remote(
            ysum.at[:, pl.ds(pl.multiple_of(zz * rows_z, 8), rows_z), :],
            rz.at[dz - 1], zsend.at[dz - 1], zrecv.at[dz - 1], me + 8 * (zz - z),
        )
        cp.start()
        zcopies.append(cp)
    total = ysum[:, pl.ds(pl.multiple_of(z * rows_z, 8), rows_z), :]
    for dz in range(1, nz):
        zcopies[dz - 1].wait_recv()
        total = total + rz[dz - 1]
    tok = tokens // n
    for k in range(8):
        for half in range(2):
            fbuf[k, :, half * half_w:(half + 1) * half_w] = total[half, k * tok:(k + 1) * tok, :]
    q = me % 8
    fcopies = []
    for dk in range(1, 8):
        k = (q + dk) % 8
        cp = remote(fbuf.at[k], gbuf.at[q], fsend.at[k], frecv.at[q], me - q + k)
        cp.start()
        fcopies.append(cp)
    gbuf[q] = fbuf[q]
    for dk in range(1, 8):
        k = (q + dk) % 8
        remote(gbuf.at[k], gbuf.at[k], fsend.at[k], frecv.at[k], me - q + k).wait_recv()
    for k in range(8):
        result[:, k * wide:(k + 1) * wide] = gbuf[k].astype(BF16)

    for group in (core_copies, stage1, stage2, zcopies, fcopies):
        for cp in group:
            cp.wait_send()

    def drain(i, carry):
        for c in range(chunks):
            exchange(c, (me + i) % n, me).wait_send()
        w_copy((me + i) % n, me).wait_send()
        v_copy((me + i) % n, me).wait_send()
        return carry

    lax.fori_loop(1, n, drain, 0)


def fused_tail(n, pix, wp, var, qtile, key_w, value_t, out_w):
    vs, tokens, patch = pix.shape
    slots = vs * n
    dl = D // n
    lanes = dl // 128
    hs = HEADS // n
    chunks = tokens // CH
    nz = n // 8
    wide = D // 8
    half_w = wide // 2
    tok = tokens // n
    dma = pltpu.SemaphoreType.DMA
    vmem = pl.BlockSpec(memory_space=pltpu.VMEM)
    hbm = pl.BlockSpec(memory_space=pl.ANY)
    return pl.pallas_call(
        functools.partial(tail_kernel, n),
        out_shape=jax.ShapeDtypeStruct((tok, D), BF16),
        in_specs=[vmem] * 4 + [hbm] * 3,
        out_specs=vmem,
        scratch_shapes=[
            pltpu.VMEM(key_w.shape, BF16),
            pltpu.VMEM((n, HEADS, dl), F32),
            pltpu.VMEM((n, vs + 1, patch, dl), BF16),
            pltpu.VMEM((n, vs, 1, dl), F32),
            pltpu.VMEM((vs * tokens, D), BF16),
            pltpu.VMEM((n, vs * tokens // 2, 2 * HEADS), F32),
            pltpu.VMEM((slots * tokens // 2, 2 * HEADS), F32),
            pltpu.VMEM((lanes, tokens * slots, 128), F32),
            pltpu.VMEM((lanes, HEADS * CH, 128), F32),
            pltpu.VMEM((chunks, HEADS * CH, dl), BF16),
            pltpu.VMEM((n, chunks, hs * CH, dl), BF16),
            pltpu.VMEM(value_t.shape, BF16),
            pltpu.VMEM(out_w.shape, BF16),
            pltpu.VMEM((2, 2, 2, 2, tokens, half_w), F32),
            pltpu.VMEM((2, 2, 2, tokens, half_w), F32),
            pltpu.VMEM((2, 2, tokens, half_w), F32),
            pltpu.VMEM((2, tokens, half_w), F32),
            pltpu.VMEM((2, tokens, half_w), F32),
            pltpu.VMEM((nz - 1, 2, tokens // nz, half_w), F32),
            pltpu.VMEM((8, tok, wide), F32),
            pltpu.VMEM((8, tok, wide), F32),
            dma((nz + 7,)), dma((nz + 7,)), dma((nz + 7,)), dma((nz + 7,)),
            dma((n,)), dma((n,)), dma((n,)), dma((n,)), dma((1,)),
            dma((2,)), dma((chunks, n)), dma((chunks, n)),
            dma((2,)), dma((2,)), dma((2,)), dma((2,)), dma((2,)), dma((2,)),
            dma((nz - 1,)), dma((nz - 1,)), dma((8,)), dma((8,)),
        ],
        compiler_params=pltpu.CompilerParams(
            has_side_effects=True, vmem_limit_bytes=60 * 1024 * 1024
        ),
    )(pix, wp, var, qtile, key_w, value_t, out_w)


def plain_body(pixels, embed_w, var_embed, key_w, query, value_t, out_w):
    group_size = lax.axis_size("dev")
    own_embed = jnp.einsum("vtp,vpd->vtd", pixels, embed_w, preferred_element_type=jnp.float32)
    own_embed = (own_embed + var_embed.astype(jnp.float32)[:, None, :]).astype(jnp.bfloat16)
    grouped = lax.all_to_all(own_embed, "dev", split_axis=1, concat_axis=0, tiled=True)
    key_rows = key_w.shape[0]
    keyq_part = jnp.einsum(
        "dhj,hj->dh",
        key_w.astype(jnp.float32).reshape(key_rows, HEADS, HD),
        query.reshape(HEADS, HD),
        precision=lax.Precision.HIGHEST,
    )
    keyq = lax.all_gather(keyq_part, "dev", axis=0, tiled=True)
    logits = jnp.einsum(
        "vtd,dh->vth", grouped.astype(jnp.float32), keyq, precision=lax.Precision.HIGHEST
    ) / jnp.sqrt(jnp.float32(HD))
    slot = lax.broadcasted_iota(jnp.int32, logits.shape, 0)
    logits = jnp.where(slot < V, logits, -1e30)
    row_max = jnp.max(logits, axis=0, keepdims=True)
    weights = jnp.exp(logits - row_max)
    attn = (weights / jnp.sum(weights, axis=0, keepdims=True)).astype(jnp.bfloat16)
    pooled = jnp.einsum("vth,vtd->thd", attn, grouped, preferred_element_type=jnp.float32).astype(
        jnp.bfloat16
    )
    own_tokens = pooled.shape[0]
    if group_size >= HEADS:
        spread = jnp.repeat(pooled, group_size // HEADS, axis=1)[:, :, None, :]
    else:
        spread = pooled.reshape(own_tokens, group_size, HEADS // group_size, D)
    received = lax.all_to_all(spread, "dev", split_axis=1, concat_axis=0, tiled=True)
    all_tokens = received.shape[0]
    head_share = received.shape[2]
    received = received.reshape(all_tokens, head_share, D)
    columns = value_t.shape[0]
    value_heads = jnp.einsum(
        "thd,hcd->thc",
        received,
        value_t.reshape(head_share, columns // head_share, D),
        preferred_element_type=jnp.float32,
    )
    value_heads = value_heads.reshape(all_tokens, columns).astype(jnp.bfloat16)
    summed = lax.psum_scatter(
        jnp.dot(value_heads, out_w, preferred_element_type=jnp.float32),
        "dev",
        scatter_dimension=0,
        tiled=True,
    )
    return summed.astype(jnp.bfloat16)


def body(pixels, embed_w, var_embed, key_w, query, value_t, out_w):
    n = lax.axis_size("dev")
    vs, tokens, patch = pixels.shape
    dl = D // n
    fits = (
        n % 8 == 0 and n // 8 >= 2 and HEADS % n == 0 and dl == 2 * HD and patch % 16 == 0
        and tokens % CH == 0 and tokens % (8 * (n // 8)) == 0 and vs * tokens <= dl
    )
    if not fits:
        return plain_body(pixels, embed_w, var_embed, key_w, query, value_t, out_w)
    turned = jnp.transpose(pixels, (2, 0, 1)).reshape(patch, vs * tokens)
    turned = jnp.pad(turned, ((0, 0), (0, dl - vs * tokens)))
    wp = jnp.concatenate([embed_w, jnp.tile(turned, (1, n))[None]], axis=0)
    hi = lax.reduce_precision(query, 8, 7)
    mid = lax.reduce_precision(query - hi, 8, 7)
    low = query - hi - mid
    parts = jnp.stack([hi, mid, low]).reshape(3, HEADS // 2, 1, 2, HD)
    own = jnp.eye(2, dtype=F32)[None, None, :, :, None]
    qtile = (parts * own).transpose(1, 0, 2, 3, 4).reshape(HEADS // 2, 6, 2 * HD)
    qtile = jnp.pad(qtile, ((0, 0), (0, 10), (0, 0))).astype(BF16)
    return fused_tail(n, pixels, wp, var_embed.astype(F32)[:, None, :], qtile, key_w, value_t, out_w)


def solution(mesh):
    placed = (
        P("dev", None, None),
        P("dev", None, None),
        P("dev", None),
        P("dev", None),
        P(),
        P("dev", None),
        P("dev", None),
    )
    return jax.shard_map(
        body, mesh=mesh, in_specs=placed, out_specs=P("dev", None), check_vma=False
    )
```

```python
import functools

import jax
import jax.numpy as jnp
from jax import lax
from jax.experimental import pallas as pl
from jax.experimental.pallas import tpu as pltpu
from jax.sharding import PartitionSpec as P

D = 8192
HEADS = 64
HD = 128
V = 91
CH = 16
EARLY = 8
MESH = pl.DeviceIdType.MESH
F32 = jnp.float32
BF16 = jnp.bfloat16


def remote(src, dst, ss, rs, dev):
    return pltpu.make_async_remote_copy(
        src_ref=src, dst_ref=dst, send_sem=ss, recv_sem=rs, device_id=(dev,), device_id_type=MESH
    )


def slot_of(s, nz):
    return (s % 2 * 4 + (s // 4) % 2 * 2 + (s // 2) % 2) * nz + s // 8


def gather_steps(buf, send, recv, me, nz):
    core, x, y, z = me % 2, (me // 2) % 2, (me // 4) % 2, me // 8
    q, qx, qy, qd = (
        core * 4 + yy * 2 + xx for yy, xx in ((y, x), (y, 1 - x), (1 - y, x), (1 - y, 1 - x))
    )
    xn, yn, other = me + 2 * (1 - 2 * x), me + 4 * (1 - 2 * y), me + 1 - 2 * core
    started = []

    def go(k, block, dev):
        cp = remote(block, block, send.at[k], recv.at[k], dev)
        cp.start()
        started.append(cp)
        return cp

    def along_z():
        for dz in range(1, nz):
            go(dz - 1, buf.at[q * nz + z], me + 8 * ((z + dz) % nz - z))

    def rest():
        for dz in range(1, nz):
            started[dz - 1].wait_recv()
        k = nz - 1
        half = nz // 2
        own = buf.at[pl.ds(q * nz, nz)]
        cx = go(k, own, xn)
        cy = go(k + 1, own, yn)
        c0 = go(k + 2, own, other)
        cx.wait_recv()
        fy = go(k + 3, buf.at[pl.ds(qx * nz, half)], yn)
        c1 = go(k + 5, buf.at[pl.ds(qx * nz, nz)], other)
        cy.wait_recv()
        fx = go(k + 4, buf.at[pl.ds(qy * nz + half, nz - half)], xn)
        c2 = go(k + 6, buf.at[pl.ds(qy * nz, nz)], other)
        return fy, fx, c0, c1, c2

    def diagonal(fy, fx, c0, c1, c2):
        fy.wait_recv()
        fx.wait_recv()
        return c0, c1, c2, go(nz + 6, buf.at[pl.ds(qd * nz, nz)], other)

    def finish(copies):
        for cp in copies:
            cp.wait_recv()
        for cp in started:
            cp.wait_send()

    return along_z, rest, diagonal, finish


def tail_kernel(
    n, pix, wp, var, qtile, key_hbm, value_hbm, out_hbm, result,
    kbuf, kq, wall, vall, oemb, lg, prob,
    embf, pf, pool, got, vbuf, obuf, part, rc, r1, r2, ysum, rz, fbuf, gbuf,
    gsend, grecv, hsend, hrecv, wsnd, wrcv, vsnd, vrcv, ksem,
    wsem, psend, precv, csend, crecv, s1send, s1recv, s2send, s2recv, zsend, zrecv, fsend, frecv,
):
    me = lax.axis_index("dev")
    core, x, y, z = me % 2, (me // 2) % 2, (me // 4) % 2, me // 8
    nz = n // 8
    vs, tokens, patch = pix.shape
    slots = n * vs
    dl = D // n
    lanes = dl // 128
    hs = HEADS // n
    chunks = tokens // CH
    take = hs * CH
    ht = tokens // 2
    mine = slot_of(me, nz)
    load_k = pltpu.make_async_copy(key_hbm, kbuf, ksem.at[0])
    load_k.start()
    load_v = pltpu.make_async_copy(value_hbm, vbuf, wsem.at[0])
    load_o = pltpu.make_async_copy(out_hbm, obuf, wsem.at[1])

    def cols_of(s):
        return pl.ds(pl.multiple_of(s * dl, 128), dl)

    def w_copy(partner, src):
        return remote(wp.at[:, :, cols_of(partner)], wall.at[src], wsnd.at[partner], wrcv.at[src], partner)

    def v_copy(partner, src):
        return remote(var.at[:, :, cols_of(partner)], vall.at[src], vsnd.at[partner], vrcv.at[src], partner)

    def w_send(i, carry):
        partner = (me + n // 2 + i) % n
        w_copy(partner, me).start()
        v_copy(partner, me).start()
        return carry

    early = EARLY
    lax.fori_loop(0, early, w_send, 0)
    load_k.wait()
    load_v.start()
    load_o.start()
    for kt in range(HEADS // 2):
        r = lax.dot_general(
            qtile[kt], kbuf[:, kt * 2 * HD:(kt + 1) * 2 * HD], (((1,), (1,)), ((), ())),
            preferred_element_type=F32,
        )
        kq[mine, 2 * kt:2 * kt + 2, :] = r[0:2] + r[2:4] + r[4:6]
    kq_z, kq_rest, kq_diag, kq_finish = gather_steps(kq, gsend, grecv, me, nz)
    lg_z, lg_rest, lg_diag, lg_finish = gather_steps(lg, hsend, hrecv, me, nz)
    kq_z()

    def own_one(s, carry):
        cols = cols_of(s)
        for v in range(vs):
            e = jnp.dot(pix[v], wp[v, :, cols], preferred_element_type=F32) + var[v, :, cols]
            oemb[v * tokens:(v + 1) * tokens, cols] = e.astype(BF16)
        return carry

    lax.fori_loop(0, n // 2, own_one, 0)
    state = kq_rest()
    lax.fori_loop(n // 2, n, own_one, 0)
    wall[me] = wp[:, :, cols_of(me)]
    vall[me] = var[:, :, cols_of(me)]
    state = kq_diag(*state)
    lax.fori_loop(early, n // 2, w_send, 0)
    lax.fori_loop(n // 2 + 1, n, w_send, 0)

    def logit_one(slot, acc):
        place = slot // nz
        s = slot % nz * 8 + (place // 2) % 2 * 4 + place % 2 * 2 + place // 4
        a = kq[slot]
        hi = a.astype(BF16)
        rest = a - hi.astype(F32)
        mid = rest.astype(BF16)
        low = (rest - mid.astype(F32)).astype(BF16)
        b = jnp.concatenate([hi, mid, low], axis=0)
        return acc + lax.dot_general(
            oemb[:, cols_of(s)], b, (((1,), (1,)), ((), ())), preferred_element_type=F32
        )

    half_n = 4 * nz
    acc = jnp.zeros((vs * tokens, 3 * HEADS), F32)
    acc = lax.fori_loop(0, half_n, lambda i, a: logit_one(core * half_n + i, a), acc)
    kq_finish(state)
    acc = lax.fori_loop(0, half_n, lambda i, a: logit_one((1 - core) * half_n + i, a), acc)
    logit = (acc[:, :HEADS] + acc[:, HEADS:2 * HEADS] + acc[:, 2 * HEADS:]) / jnp.sqrt(F32(HD))
    for v in range(vs):
        pair = jnp.concatenate(
            [logit[v * tokens:v * tokens + ht], logit[v * tokens + ht:(v + 1) * tokens]], axis=1
        )
        live = jnp.full(pair.shape, me * vs + v, jnp.int32) < V
        lg[mine, v * ht:(v + 1) * ht, :] = jnp.where(live, pair, -1e30)
    lg_z()

    def embed_one(s):
        ps = jnp.transpose(wall[s, vs].astype(F32)).astype(BF16)
        at = slot_of(s, nz) * vs
        for v in range(vs):
            e = jnp.dot(ps[v * tokens:(v + 1) * tokens], wall[s, v], preferred_element_type=F32) + vall[s, v]
            e = e.astype(BF16).astype(F32)
            for k in range(lanes):
                embf[k, pl.ds(at + v, tokens, stride=slots), :] = e[:, k * 128:(k + 1) * 128]

    def arrive_w(i, carry):
        s = (me + n + n // 2 - i) % n
        w_copy(s, s).wait_recv()
        v_copy(s, s).wait_recv()
        embed_one(s)
        return carry

    embed_one(me)
    lax.fori_loop(0, early, arrive_w, 0)
    state = lg_rest()
    lax.fori_loop(early, n // 2, arrive_w, 0)
    state = lg_diag(*state)
    lax.fori_loop(n // 2 + 1, n, arrive_w, 0)
    lg_finish(state)
    def top_one(k, top):
        for v in range(vs):
            top = jnp.maximum(top, lg[k, v * ht:(v + 1) * ht, :])
        return top

    top = lax.fori_loop(0, n, top_one, lg[0, :ht, :], unroll=4)

    def exp_one(k, total):
        for v in range(vs):
            e = jnp.exp(lg[k, v * ht:(v + 1) * ht, :] - top)
            prob[pl.ds(pl.multiple_of((k * vs + v) * ht, 8), ht), :] = e
            total = total + e
        return total

    total = lax.fori_loop(0, n, exp_one, jnp.zeros((ht, 2 * HEADS), F32), unroll=2)

    def div_one(k, carry):
        for v in range(vs):
            rows = pl.ds(pl.multiple_of((k * vs + v) * ht, 8), ht)
            prob[rows, :] = prob[rows, :] / total
        return carry

    lax.fori_loop(0, n, div_one, 0, unroll=2)

    def exchange(c, partner, slot):
        return pltpu.make_async_remote_copy(
            src_ref=pool.at[c, pl.ds(pl.multiple_of(partner * take, 16), take), :],
            dst_ref=got.at[slot, c],
            send_sem=psend.at[c, partner],
            recv_sem=precv.at[c, slot],
            device_id=(partner,),
            device_id_type=MESH,
        )

    for c in range(chunks):
        def pool_one(tt, carry, c=c):
            t = c * (CH // 2) + tt
            at = prob[pl.ds(t, slots, stride=ht), :].astype(BF16)
            for side in range(2):
                row = pl.ds(pl.multiple_of((t + side * ht) * slots, 8), slots)
                em = jnp.concatenate([embf[k, row, :] for k in range(lanes)], axis=1).astype(BF16)
                p = lax.dot_general(
                    at[:, side * HEADS:(side + 1) * HEADS], em, (((0,), (0,)), ((), ())),
                    preferred_element_type=F32,
                )
                for k in range(lanes):
                    pf[k, pl.ds(tt + side * (CH // 2), HEADS, stride=CH), :] = p[:, k * 128:(k + 1) * 128]
            return carry

        lax.fori_loop(0, CH // 2, pool_one, 0, unroll=2)

        def pack(i, carry, c=c):
            rows = pl.ds(pl.multiple_of(i * 64, 64), 64)
            pool[c, rows, :] = jnp.concatenate([pf[k, rows, :] for k in range(lanes)], axis=1).astype(BF16)
            return carry

        lax.fori_loop(0, HEADS * CH // 64, pack, 0)
        got[me, c] = pool[c, pl.ds(pl.multiple_of(me * take, 16), take), :]

        def send(i, carry, c=c):
            exchange(c, (me + n // 2 + i) % n, me).start()
            return carry

        lax.fori_loop(0, n // 2, send, 0)
        lax.fori_loop(n // 2 + 1, n, send, 0)

    load_v.wait()

    def value_one(i, accs):
        s = (me + i) % n
        block = got[s]
        cols = pl.ds(pl.multiple_of(s * dl, 128), dl)
        new = []
        for h in range(hs):
            r = block[:, h * CH:(h + 1) * CH, :].reshape(tokens, dl)
            vv = vbuf[h * HD:(h + 1) * HD, cols]
            new.append(accs[h] + lax.dot_general(r, vv, (((1,), (1,)), ((), ())), preferred_element_type=F32))
        return tuple(new)

    def arrive_one(i, accs):
        s = (me + i) % n
        for c in range(chunks):
            pltpu.make_async_remote_copy(
                src_ref=got.at[s, c], dst_ref=got.at[s, c], send_sem=psend.at[c, s],
                recv_sem=precv.at[c, s], device_id=(s,), device_id_type=MESH,
            ).wait_recv()
        return value_one(i, accs)

    accs = value_one(0, tuple(jnp.zeros((tokens, HD), F32) for _ in range(hs)))
    accs = lax.fori_loop(1, n, arrive_one, accs)
    heads = jnp.concatenate(accs, axis=1)
    hc = CH // 2
    heads = jnp.concatenate(
        [heads[c * CH + side * hc:c * CH + (side + 1) * hc] for side in range(2) for c in range(chunks)], axis=0
    ).astype(BF16)

    load_o.wait()
    wide = D // 8
    half_w = wide // 2

    def out_blocks(cc, half):
        for a in range(2):
            for b in range(2):
                q = cc + 2 * (a if half == 0 else b) + 4 * (b if half == 0 else a)
                col = pl.multiple_of(q * wide + half * half_w, 128)
                part[cc, half, a, b] = jnp.dot(heads, obuf[:, pl.ds(col, half_w)], preferred_element_type=F32)

    other = me + 1 - 2 * core
    xn = me + 2 * (1 - 2 * x)
    yn = me + 4 * (1 - 2 * y)
    core_copies = []
    for half in range(2):
        out_blocks(1 - core, half)
        cp = remote(part.at[1 - core, half], rc.at[half], csend.at[half], crecv.at[half], other)
        cp.start()
        core_copies.append(cp)
    for half in range(2):
        out_blocks(core, half)
    first = (x, y)
    second = (y, x)
    first_dev = (xn, yn)
    second_dev = (yn, xn)
    stage1 = []
    for half in range(2):
        core_copies[half].wait_recv()
        away = 1 - first[half]
        for b in range(2):
            part[core, half, away, b] = part[core, half, away, b] + rc[half, away, b]
        cp = remote(part.at[core, half, away], r1.at[half], s1send.at[half], s1recv.at[half], first_dev[half])
        cp.start()
        stage1.append(cp)
    for half in range(2):
        own = first[half]
        for b in range(2):
            part[core, half, own, b] = part[core, half, own, b] + rc[half, own, b]
    stage2 = []
    for half in range(2):
        own = first[half]
        stage1[half].wait_recv()
        away = 1 - second[half]
        part[core, half, own, away] = part[core, half, own, away] + r1[half, away]
        cp = remote(part.at[core, half, own, away], r2.at[half], s2send.at[half], s2recv.at[half], second_dev[half])
        cp.start()
        stage2.append(cp)
    for half in range(2):
        own, kept_b = first[half], second[half]
        kept = part[core, half, own, kept_b] + r1[half, kept_b]
        stage2[half].wait_recv()
        ysum[half] = kept + r2[half]
    rows_z = tokens // nz
    zcopies = []
    for dz in range(1, nz):
        zz = (z + dz) % nz
        cp = remote(
            ysum.at[:, pl.ds(pl.multiple_of(zz * rows_z, 8), rows_z), :],
            rz.at[dz - 1], zsend.at[dz - 1], zrecv.at[dz - 1], me + 8 * (zz - z),
        )
        cp.start()
        zcopies.append(cp)
    total = ysum[:, pl.ds(pl.multiple_of(z * rows_z, 8), rows_z), :]
    for dz in range(1, nz):
        zcopies[dz - 1].wait_recv()
        total = total + rz[dz - 1]
    tok = tokens // n
    for k in range(8):
        for half in range(2):
            fbuf[k, :, half * half_w:(half + 1) * half_w] = total[half, k * tok:(k + 1) * tok, :]
    q = me % 8
    fcopies = []
    for dk in range(1, 8):
        k = (q + dk) % 8
        cp = remote(fbuf.at[k], gbuf.at[q], fsend.at[k], frecv.at[q], me - q + k)
        cp.start()
        fcopies.append(cp)
    gbuf[q] = fbuf[q]
    for dk in range(1, 8):
        k = (q + dk) % 8
        remote(gbuf.at[k], gbuf.at[k], fsend.at[k], frecv.at[k], me - q + k).wait_recv()
    for k in range(8):
        result[:, k * wide:(k + 1) * wide] = gbuf[k].astype(BF16)

    for group in (core_copies, stage1, stage2, zcopies, fcopies):
        for cp in group:
            cp.wait_send()

    def drain(i, carry):
        for c in range(chunks):
            exchange(c, (me + i) % n, me).wait_send()
        w_copy((me + i) % n, me).wait_send()
        v_copy((me + i) % n, me).wait_send()
        return carry

    lax.fori_loop(1, n, drain, 0)


def fused_tail(n, pix, wp, var, qtile, key_w, value_t, out_w):
    vs, tokens, patch = pix.shape
    slots = vs * n
    dl = D // n
    lanes = dl // 128
    hs = HEADS // n
    chunks = tokens // CH
    nz = n // 8
    wide = D // 8
    half_w = wide // 2
    tok = tokens // n
    dma = pltpu.SemaphoreType.DMA
    vmem = pl.BlockSpec(memory_space=pltpu.VMEM)
    hbm = pl.BlockSpec(memory_space=pl.ANY)
    return pl.pallas_call(
        functools.partial(tail_kernel, n),
        out_shape=jax.ShapeDtypeStruct((tok, D), BF16),
        in_specs=[vmem] * 4 + [hbm] * 3,
        out_specs=vmem,
        scratch_shapes=[
            pltpu.VMEM(key_w.shape, BF16),
            pltpu.VMEM((n, HEADS, dl), F32),
            pltpu.VMEM((n, vs + 1, patch, dl), BF16),
            pltpu.VMEM((n, vs, 1, dl), F32),
            pltpu.VMEM((vs * tokens, D), BF16),
            pltpu.VMEM((n, vs * tokens // 2, 2 * HEADS), F32),
            pltpu.VMEM((slots * tokens // 2, 2 * HEADS), F32),
            pltpu.VMEM((lanes, tokens * slots, 128), F32),
            pltpu.VMEM((lanes, HEADS * CH, 128), F32),
            pltpu.VMEM((chunks, HEADS * CH, dl), BF16),
            pltpu.VMEM((n, chunks, hs * CH, dl), BF16),
            pltpu.VMEM(value_t.shape, BF16),
            pltpu.VMEM(out_w.shape, BF16),
            pltpu.VMEM((2, 2, 2, 2, tokens, half_w), F32),
            pltpu.VMEM((2, 2, 2, tokens, half_w), F32),
            pltpu.VMEM((2, 2, tokens, half_w), F32),
            pltpu.VMEM((2, tokens, half_w), F32),
            pltpu.VMEM((2, tokens, half_w), F32),
            pltpu.VMEM((nz - 1, 2, tokens // nz, half_w), F32),
            pltpu.VMEM((8, tok, wide), F32),
            pltpu.VMEM((8, tok, wide), F32),
            dma((nz + 7,)), dma((nz + 7,)), dma((nz + 7,)), dma((nz + 7,)),
            dma((n,)), dma((n,)), dma((n,)), dma((n,)), dma((1,)),
            dma((2,)), dma((chunks, n)), dma((chunks, n)),
            dma((2,)), dma((2,)), dma((2,)), dma((2,)), dma((2,)), dma((2,)),
            dma((nz - 1,)), dma((nz - 1,)), dma((8,)), dma((8,)),
        ],
        compiler_params=pltpu.CompilerParams(
            has_side_effects=True, vmem_limit_bytes=60 * 1024 * 1024
        ),
    )(pix, wp, var, qtile, key_w, value_t, out_w)


def plain_body(pixels, embed_w, var_embed, key_w, query, value_t, out_w):
    group_size = lax.axis_size("dev")
    own_embed = jnp.einsum("vtp,vpd->vtd", pixels, embed_w, preferred_element_type=jnp.float32)
    own_embed = (own_embed + var_embed.astype(jnp.float32)[:, None, :]).astype(jnp.bfloat16)
    grouped = lax.all_to_all(own_embed, "dev", split_axis=1, concat_axis=0, tiled=True)
    key_rows = key_w.shape[0]
    keyq_part = jnp.einsum(
        "dhj,hj->dh",
        key_w.astype(jnp.float32).reshape(key_rows, HEADS, HD),
        query.reshape(HEADS, HD),
        precision=lax.Precision.HIGHEST,
    )
    keyq = lax.all_gather(keyq_part, "dev", axis=0, tiled=True)
    logits = jnp.einsum(
        "vtd,dh->vth", grouped.astype(jnp.float32), keyq, precision=lax.Precision.HIGHEST
    ) / jnp.sqrt(jnp.float32(HD))
    slot = lax.broadcasted_iota(jnp.int32, logits.shape, 0)
    logits = jnp.where(slot < V, logits, -1e30)
    row_max = jnp.max(logits, axis=0, keepdims=True)
    weights = jnp.exp(logits - row_max)
    attn = (weights / jnp.sum(weights, axis=0, keepdims=True)).astype(jnp.bfloat16)
    pooled = jnp.einsum("vth,vtd->thd", attn, grouped, preferred_element_type=jnp.float32).astype(
        jnp.bfloat16
    )
    own_tokens = pooled.shape[0]
    if group_size >= HEADS:
        spread = jnp.repeat(pooled, group_size // HEADS, axis=1)[:, :, None, :]
    else:
        spread = pooled.reshape(own_tokens, group_size, HEADS // group_size, D)
    received = lax.all_to_all(spread, "dev", split_axis=1, concat_axis=0, tiled=True)
    all_tokens = received.shape[0]
    head_share = received.shape[2]
    received = received.reshape(all_tokens, head_share, D)
    columns = value_t.shape[0]
    value_heads = jnp.einsum(
        "thd,hcd->thc",
        received,
        value_t.reshape(head_share, columns // head_share, D),
        preferred_element_type=jnp.float32,
    )
    value_heads = value_heads.reshape(all_tokens, columns).astype(jnp.bfloat16)
    summed = lax.psum_scatter(
        jnp.dot(value_heads, out_w, preferred_element_type=jnp.float32),
        "dev",
        scatter_dimension=0,
        tiled=True,
    )
    return summed.astype(jnp.bfloat16)


def body(pixels, embed_w, var_embed, key_w, query, value_t, out_w):
    n = lax.axis_size("dev")
    vs, tokens, patch = pixels.shape
    dl = D // n
    fits = (
        n % 8 == 0 and n // 8 >= 2 and HEADS % n == 0 and dl == 2 * HD and patch % 16 == 0
        and tokens % CH == 0 and tokens % (8 * (n // 8)) == 0 and vs * tokens <= dl
    )
    if not fits:
        return plain_body(pixels, embed_w, var_embed, key_w, query, value_t, out_w)
    turned = jnp.transpose(pixels, (2, 0, 1)).reshape(patch, vs * tokens)
    turned = jnp.pad(turned, ((0, 0), (0, dl - vs * tokens)))
    wp = jnp.concatenate([embed_w, jnp.tile(turned, (1, n))[None]], axis=0)
    hi = lax.reduce_precision(query, 8, 7)
    mid = lax.reduce_precision(query - hi, 8, 7)
    low = query - hi - mid
    parts = jnp.stack([hi, mid, low]).reshape(3, HEADS // 2, 1, 2, HD)
    own = jnp.eye(2, dtype=F32)[None, None, :, :, None]
    qtile = (parts * own).transpose(1, 0, 2, 3, 4).reshape(HEADS // 2, 6, 2 * HD)
    qtile = jnp.pad(qtile, ((0, 0), (0, 10), (0, 0))).astype(BF16)
    return fused_tail(n, pixels, wp, var_embed.astype(F32)[:, None, :], qtile, key_w, value_t, out_w)


def solution(mesh):
    placed = (
        P("dev", None, None),
        P("dev", None, None),
        P("dev", None),
        P("dev", None),
        P(),
        P("dev", None),
        P("dev", None),
    )
    return jax.shard_map(
        body, mesh=mesh, in_specs=placed, out_specs=P("dev", None), check_vma=False
    )
```
